512 devices in a mesh: dp: 8 (over x, core), vocab: 64 (over y, z).
Axes of the slice: x: 4, y: 8, z: 8, core: 2. Of those that a mesh axis runs over, the one named last changes fastest.
Arguments:
- hidden: bfloat16 [1792, 4608], P('dp'), may hold values from -15 to 15
- out_weight: bfloat16 [4608, 24576], P('dp', 'vocab'), may hold values from -0.09375 to 0.09375
- targets: int32 [1792], P('dp'), may hold values from 0 to 24383
- token_weight: float32 [1792], P('dp'), may hold values from 0.3 to 3
Outputs:
- token_loss: float32 [1792], P('dp')
- hidden_grad: bfloat16 [1792, 4608], P('dp')
- weight_grad: bfloat16 [4608, 24576], P('dp', 'vocab')
The draws below stay inside these ranges and needn't reach their ends.
All inputs are finite; a program needn't handle non-finite values.
Results may differ from the reference program's by a relative error of at most 0.0085.
Values may be sent and summed in bfloat16 or wider, within the bound.
A program may use at most 64 MiB of HBM per device.

```python
import math
import jax
import jax.numpy as jnp
from jax import lax

D = 4608
VOCAB_DEV = 384
TOK_DEV = 224
TOKENS = 1792
VOCAB_PAD = 24576
VOCAB = 24384
N_DP = 8
N_VOCAB = 64


def touch_ends(drawn, own_key, smallest, largest):
    index_at = [jax.random.randint(jax.random.fold_in(own_key, axis), (), 0, length) for axis, length in enumerate(drawn.shape)]
    longest = drawn.shape.index(max(drawn.shape))
    beside = index_at[:longest] + [(index_at[longest] + 1) % drawn.shape[longest]] + index_at[longest + 1:]
    return drawn.at[tuple(index_at)].set(smallest).at[tuple(beside)].set(largest)


def block_scale(own_key, shape, cuts, smallest, high):
    factor_of = 1.0
    for position, shards_of in cuts:
        steps = jax.random.uniform(jax.random.fold_in(jax.random.fold_in(own_key, 6), position), (shards_of,), jnp.float32, smallest / len(cuts), high / len(cuts))
        factor_of = factor_of * jnp.repeat(jnp.exp(steps), shape[position] // shards_of).reshape((-1,) + (1,) * (len(shape) - 1 - position))
    return factor_of


def gaussian(rng, dims, width, limit, shards=(), held_as=jnp.bfloat16):
    drawn = jax.random.normal(rng, dims, jnp.float32) * width
    if len(shards) > 0:
        drawn = block_scale(rng, dims, shards, -0.22, 0.18) * drawn
    return jnp.clip(drawn, min=-limit, max=limit).astype(held_as)


def setup_inputs(seed: int = 0) -> dict:
    streams_of = jax.random.split(jax.random.key(seed), 5)
    hidden = gaussian(streams_of[0], (TOKENS, D), 3.0, 15.0, ((0, 8),))
    out_weight = gaussian(streams_of[1], (D, VOCAB_PAD), D ** -0.5, 0.09375, ((0, 8), (1, 64)))
    targets = touch_ends(jax.random.randint(streams_of[2], (TOKENS,), 0, VOCAB), jax.random.fold_in(streams_of[2], 1), 0, VOCAB - 1).astype(jnp.int32)
    token_weight = jnp.clip(jnp.exp(math.log(3.0) - 2.3025851 * jax.random.uniform(streams_of[3], (TOKENS,), jnp.float32) ** block_scale(streams_of[3], (TOKENS,), ((0, 8),), -0.2, 0.2)), 0.3, 3.0)
    return dict(hidden=hidden, out_weight=out_weight, targets=targets, token_weight=token_weight)


softcap = 30.0


def reference(hidden, out_weight, targets, token_weight):
    padded = VOCAB_DEV * N_VOCAB
    logits = jnp.dot(hidden, out_weight, preferred_element_type=jnp.float32)
    squash = jnp.tanh(logits / softcap)
    capped = softcap * squash
    col_ids = jnp.arange(padded, dtype=jnp.int32)
    usable = col_ids < VOCAB
    exp_terms = jnp.where(usable[None, :], jnp.exp(capped), jnp.float32(0.0))
    sums = jnp.sum(exp_terms, axis=1)
    target_hit = col_ids[None, :] == targets[:, None].astype(jnp.int32)
    target_logit = jnp.sum(jnp.where(target_hit, capped, jnp.float32(0.0)), axis=1)
    token_loss = jnp.log(sums) - target_logit
    onehot = jnp.where(target_hit, jnp.float32(1.0), jnp.float32(0.0))
    logit_grad = (token_weight[:, None] * (exp_terms / sums[:, None] - onehot) * (1.0 - squash * squash)).astype(jnp.bfloat16)
    hidden_grad = jnp.dot(logit_grad, out_weight.T, preferred_element_type=jnp.float32).astype(jnp.bfloat16)
    hidden_blocks = hidden.reshape(N_DP, TOK_DEV, D)
    grad_blocks = logit_grad.reshape(N_DP, TOK_DEV, padded)

    def add_block(carried, pair):
        block_term = jnp.dot(pair[0].T, pair[1], preferred_element_type=jnp.float32).astype(jnp.bfloat16)
        block_term = lax.optimization_barrier(block_term)
        return carried + block_term.astype(jnp.float32), None

    summed, _ = lax.scan(add_block, jnp.zeros((D, padded), jnp.float32), (hidden_blocks, grad_blocks))
    return token_loss, hidden_grad, summed.astype(jnp.bfloat16)
```

```python
import jax
import jax.numpy as jnp
from jax import lax
from jax.experimental import pallas as pl
from jax.experimental.pallas import tpu as pltpu
from jax.sharding import Mesh
from jax.sharding import PartitionSpec as P

MESH = pl.DeviceIdType.MESH
F32 = jnp.float32
BF16 = jnp.bfloat16

softcap = 30.0

NX = 4
NR = 8
TOK = 224
TOKP = 256
WROWS = 576
CHIP = 2 * WROWS
COLS = 384
WHALF = WROWS // 2
PROWS = TOK // 2
SUBS = CHIP // COLS
GROUPS = PROWS // 16
NT = (((1,), (1,)), ((), ()))


def kernel(
    h_ref, w_ref, t_ref, tw_ref,
    loss_ref, hg_ref, wg_ref,
    hv, ht, wf, acc, a1, a2, rows, tcol, wcol, s128, t128, st1, st2, gk,
    sp, rp, sm, rm, fb, r2, og,
    ds_, dr, xs, xr, wout,
    in_sem, out_sem, w_s, w_r, st_s, st_r, p_s, p_r, m_s, m_r, f_s, f_r, g_s, g_r,
    ap_s, ap_r, am_s, am_r, d_s, d_r, x_s, x_r,
):
    x, c = lax.axis_index("x"), lax.axis_index("c")
    y, z = lax.axis_index("y"), lax.axis_index("z")
    xl, xr_, x2 = (x + NX - 1) % NX, (x + 1) % NX, (x + 2) % NX
    oc = 1 - c
    i = y * oc + z * c
    j = z * oc + y * c

    def first(n):
        return (x, c, n * oc + y * c, z * oc + n * c)

    def second(n):
        return (x, c, y * oc + n * c, n * oc + z * c)

    right, left, partner = (xr_, c, y, z), (xl, c, y, z), (x, oc, y, z)
    sent = []

    def copy(src, dst, s, r, dev):
        return pltpu.make_async_remote_copy(
            src_ref=src, dst_ref=dst, send_sem=s, recv_sem=r, device_id=dev, device_id_type=MESH
        )

    def send(src, dst, s, r, dev):
        rc = copy(src, dst, s, r, dev)
        rc.start()
        sent.append(rc)

    def arrived(dst, s, r):
        copy(dst, dst, s, r, partner).wait_recv()

    def wpart(xx, cc, h):
        return wf.at[xx, pl.ds(pl.multiple_of(cc * WROWS + h * WHALF, 32), WHALF)]

    own_rows = pl.ds(pl.multiple_of(c * WROWS, 32), WROWS)
    other_rows = pl.ds(pl.multiple_of(oc * WROWS, 32), WROWS)

    w_in = pltpu.make_async_copy(w_ref, wf.at[x, own_rows], in_sem.at[0])
    w_in.start()
    h_in = pltpu.make_async_copy(h_ref, hv.at[pl.ds(0, TOK)], in_sem.at[1])
    h_in.start()

    barrier = pltpu.get_barrier_semaphore()
    peers = [right, left, partner]
    for k in range(1, NR):
        peers.append(first((i + k) % NR))
        peers.append(second((j + k) % NR))
    for peer in peers:
        pl.semaphore_signal(barrier, inc=1, device_id=peer, device_id_type=MESH)
    pl.semaphore_wait(barrier, len(peers))

    w_in.wait()
    send(wpart(x, c, 0), wpart(x, c, 0), w_s.at[0], w_r.at[0], right)
    send(wpart(x, c, 1), wpart(x, c, 1), w_s.at[3], w_r.at[3], left)
    send(wpart(x, c, 1), wpart(x, c, 1), w_s.at[1], w_r.at[1], right)
    send(wpart(x, c, 0), wpart(x, c, 0), w_s.at[4], w_r.at[4], left)
    send(wf.at[x, own_rows], wf.at[x, own_rows], w_s.at[6], w_r.at[6], partner)

    rows[...] = jnp.zeros_like(rows)
    rows[0:1, 0:TOK] = t_ref[...].astype(F32)
    rows[1:2, 0:TOK] = tw_ref[...]
    tcol[...] = jnp.broadcast_to(rows[0:1, :], (128, TOKP)).T.astype(jnp.int32)
    wcol[...] = jnp.broadcast_to(rows[1:2, :], (128, TOKP)).T
    s128[pl.ds(TOK, TOKP - TOK)] = jnp.zeros((TOKP - TOK, 128), F32)
    t128[pl.ds(TOK, TOKP - TOK)] = jnp.zeros((TOKP - TOK, 128), F32)
    gk[pl.ds(TOK, TOKP - TOK)] = jnp.zeros((TOKP - TOK, COLS), BF16)
    hv[pl.ds(TOK, TOKP - TOK)] = jnp.zeros((TOKP - TOK, NX * CHIP), BF16)
    h_in.wait()

    def part_logits(xx):
        at = pl.ds(pl.multiple_of(xx * CHIP, 128), CHIP)
        return jnp.dot(hv[pl.ds(0, TOK), at], wf[xx], preferred_element_type=F32)

    arrived(wf.at[x, other_rows], w_s.at[6], w_r.at[6])
    acc[...] = part_logits(x)

    @pl.loop(0, NX)
    def _(n):
        @pl.loop(0, CHIP // 128)
        def _(b):
            at = pl.ds(pl.multiple_of(n * CHIP + b * 128, 128), 128)
            ht[n, pl.ds(pl.multiple_of(b * 128, 128), 128), :] = hv[:, at].T

    arrived(wpart(xl, c, 0), w_s.at[0], w_r.at[0])
    send(wpart(xl, c, 0), wpart(xl, c, 0), w_s.at[2], w_r.at[2], right)
    send(wpart(xl, c, 0), wpart(xl, c, 0), w_s.at[7], w_r.at[7], partner)
    arrived(wpart(xr_, c, 1), w_s.at[3], w_r.at[3])
    send(wpart(xr_, c, 1), wpart(xr_, c, 1), w_s.at[5], w_r.at[5], left)
    send(wpart(xr_, c, 1), wpart(xr_, c, 1), w_s.at[8], w_r.at[8], partner)
    arrived(wpart(xl, c, 1), w_s.at[1], w_r.at[1])
    send(wpart(xl, c, 1), wpart(xl, c, 1), w_s.at[9], w_r.at[9], partner)
    arrived(wpart(xr_, c, 0), w_s.at[4], w_r.at[4])
    send(wpart(xr_, c, 0), wpart(xr_, c, 0), w_s.at[10], w_r.at[10], partner)
    arrived(wpart(xl, oc, 0), w_s.at[7], w_r.at[7])
    arrived(wpart(xl, oc, 1), w_s.at[9], w_r.at[9])
    acc[...] += part_logits(xl)
    arrived(wpart(xr_, oc, 1), w_s.at[8], w_r.at[8])
    arrived(wpart(xr_, oc, 0), w_s.at[10], w_r.at[10])
    acc[...] += part_logits(xr_)
    arrived(wpart(x2, c, 0), w_s.at[2], w_r.at[2])
    send(wpart(x2, c, 0), wpart(x2, c, 0), w_s.at[11], w_r.at[11], partner)
    arrived(wpart(x2, c, 1), w_s.at[5], w_r.at[5])
    send(wpart(x2, c, 1), wpart(x2, c, 1), w_s.at[12], w_r.at[12], partner)
    arrived(wpart(x2, oc, 0), w_s.at[11], w_r.at[11])
    arrived(wpart(x2, oc, 1), w_s.at[12], w_r.at[12])
    acc[...] += part_logits(x2)

    first_col = (y * NR + z) * COLS
    used = COLS * NR * NR - COLS // 2

    @pl.loop(0, TOK // 16)
    def _(r):
        at = pl.ds(pl.multiple_of(r * 16, 16), 16)
        tgt, wgt = tcol[at], wcol[at]
        total, hits = jnp.zeros((16, 128), F32), jnp.zeros((16, 128), F32)
        for n in range(COLS // 128):
            lanes = pl.ds(n * 128, 128)
            ids = first_col + n * 128 + lax.broadcasted_iota(jnp.int32, (16, 128), 1)
            squash = jnp.tanh(acc[at, lanes] / softcap)
            capped = softcap * squash
            exps = jnp.where(ids < used, jnp.exp(capped), 0.0)
            hit = ids == tgt
            slope = wgt * (1.0 - squash * squash)
            a1[at, lanes] = slope * exps
            a2[at, lanes] = jnp.where(hit, slope, 0.0)
            total += exps
            hits += jnp.where(hit, capped, 0.0)
        s128[at] = total
        t128[at] = hits

    st1[i, 0:1, :] = jnp.sum(s128[...].T, axis=0, keepdims=True)
    st1[i, 1:2, :] = jnp.sum(t128[...].T, axis=0, keepdims=True)

    def share(st, mine, dev, base):
        for k in range(1, NR):
            send(st.at[mine], st.at[mine], st_s.at[base + k], st_r.at[base + k], dev((mine + k) % NR))
        for k in range(1, NR):
            arrived(st.at[(mine + NR - k) % NR], st_s.at[base + k], st_r.at[base + k])
        total = st[0]
        for k in range(1, NR):
            total += st[k]
        return total

    st2[j] = share(st1, i, first, 0)
    stats = share(st2, j, second, NR)
    sums = stats[0:1, :]
    loss_ref[...] = jnp.log(sums[:, 0:TOK]) - stats[1:2, 0:TOK]
    s128[...] = jnp.broadcast_to(1.0 / sums, (128, TOKP)).T

    @pl.loop(0, TOK // 16)
    def _(r):
        at = pl.ds(pl.multiple_of(r * 16, 16), 16)
        inv = s128[at]
        for n in range(COLS // 128):
            lanes = pl.ds(n * 128, 128)
            gk[at, lanes] = (a1[at, lanes] * inv - a2[at, lanes]).astype(BF16)

    up, down = first((i + 1) % NR), first((i + NR - 1) % NR)

    def piece(p, sub):
        g = gk[pl.ds(pl.multiple_of((p // NX) * PROWS, 16), PROWS), :]
        w = wf[p % NX, pl.ds(sub * COLS, COLS), :]
        return lax.dot_general(g, w, NT, preferred_element_type=F32)

    def hop_up(s, sub):
        val = piece((i + 4 - s) % NR, sub)
        if s > 1 or (s == 1 and sub < 2):
            arrived(rp.at[s - 1, sub], p_s.at[s - 1, sub], p_r.at[s - 1, sub])
            val += rp[s - 1, sub].astype(F32)
        sp[s, sub] = val.astype(BF16)
        send(sp.at[s, sub], rp.at[s, sub], p_s.at[s, sub], p_r.at[s, sub], up)

    def hop_down(s, sub):
        val = piece((i + 4 + s) % NR, sub)
        if s > 1 or (s == 1 and sub == 2):
            arrived(rm.at[s - 1, sub], m_s.at[s - 1, sub], m_r.at[s - 1, sub])
            val += rm[s - 1, sub].astype(F32)
        sm[s, sub] = val.astype(BF16)
        send(sm.at[s, sub], rm.at[s, sub], m_s.at[s, sub], m_r.at[s, sub], down)

    hop_up(0, 0)
    hop_down(0, 2)
    hop_up(0, 1)
    hop_down(1, 0)
    hop_down(1, 1)
    hop_up(1, 2)

    def term(xx, cc, h):
        a = ht[xx, pl.ds(pl.multiple_of(cc * WROWS + h * WHALF, 32), WHALF), :]
        return jnp.dot(a, gk[...], preferred_element_type=F32)

    def give(xx, h):
        ds_[xx, h] = term(xx, oc, h).astype(BF16)
        send(ds_.at[xx, h], dr.at[xx, h], d_s.at[xx, h], d_r.at[xx, h], partner)

    def chip_term(xx, h):
        val = term(xx, c, h)
        arrived(dr.at[xx, h], d_s.at[xx, h], d_r.at[xx, h])
        return val + dr[xx, h].astype(F32)

    def pass_on(n, val, dev):
        xs[n] = val.astype(BF16)
        send(xs.at[n], xr.at[n], x_s.at[n], x_r.at[n], dev)

    def got(n):
        arrived(xr.at[n], x_s.at[n], x_r.at[n])
        return xr[n].astype(F32)

    give(x2, 0)
    give(x2, 1)
    hop_up(1, 0)
    hop_down(1, 2)
    hop_up(1, 1)
    give(xr_, 1)
    give(xl, 0)
    pass_on(0, chip_term(x2, 0), right)
    pass_on(3, chip_term(x2, 1), left)
    for sub in (0, 2, 1):
        hop_up(2, sub)
        hop_down(2, 2 - sub)
    give(xr_, 0)
    give(xl, 1)
    pass_on(1, chip_term(xr_, 1), right)
    pass_on(4, chip_term(xl, 0), left)
    for sub in (0, 2, 1):
        hop_up(3, sub)
        hop_down(3, 2 - sub)
    give(x, 0)
    give(x, 1)

    for sub in range(SUBS):
        val = piece(i, sub)
        arrived(rp.at[3, sub], p_s.at[3, sub], p_r.at[3, sub])
        arrived(rm.at[3, sub], m_s.at[3, sub], m_r.at[3, sub])
        val += rp[3, sub].astype(F32) + rm[3, sub].astype(F32)
        fb[:, :, pl.ds(sub * COLS, COLS)] = val.astype(BF16).reshape(GROUPS, 16, COLS)

    for k in range(1, NR):
        g = (j + k) % NR

        @pl.when(g < GROUPS)
        def _():
            copy(fb.at[g], r2.at[j], f_s.at[k], f_r.at[k], second(g)).start()

    pass_on(2, chip_term(xr_, 0) + got(0), right)
    pass_on(5, chip_term(xl, 1) + got(3), left)

    @pl.when(j < GROUPS)
    def _():
        total = fb[j].astype(F32)
        for k in range(1, NR):
            arrived(r2.at[(j + NR - k) % NR], f_s.at[k], f_r.at[k])
            total += r2[(j + NR - k) % NR].astype(F32)
        og[i, j] = total.astype(BF16)
        for k in range(1, NR):
            copy(og.at[i, j], og.at[i, j], g_s.at[k], g_r.at[j], second((j + k) % NR)).start()

    def ring(s, g, p_up, p_down, ups, downs):
        if ups:
            send(og.at[p_up, g], og.at[p_up, g], ap_s.at[s, g], ap_r.at[s, g], up)
        if downs:
            send(og.at[p_down, g], og.at[p_down, g], am_s.at[s, g], am_r.at[s, g], down)

    for g in range(GROUPS):
        @pl.when(j != g)
        def _():
            arrived(og.at[i, g], g_s.at[0], g_r.at[g])
        ring(0, g, i, i, True, True)

    for s in range(1, 4):
        p_up, p_down = (i + NR - s) % NR, (i + s) % NR
        for g in range(GROUPS):
            arrived(og.at[p_up, g], ap_s.at[s - 1, g], ap_r.at[s - 1, g])
            arrived(og.at[p_down, g], am_s.at[s - 1, g], am_r.at[s - 1, g])
            ring(s, g, p_up, p_down, s < 3 or g < 4, s < 3 or g >= 4)

    wout[pl.ds(0, WHALF)] = (chip_term(x, 0) + got(2) + got(4)).astype(BF16)
    wout[pl.ds(WHALF, WHALF)] = (chip_term(x, 1) + got(5) + got(1)).astype(BF16)
    w_out = pltpu.make_async_copy(wout, wg_ref, out_sem.at[NR])
    w_out.start()

    far = (i + 4) % NR
    for g in range(GROUPS):
        if g < 4:
            arrived(og.at[far, g], ap_s.at[3, g], ap_r.at[3, g])
        else:
            arrived(og.at[far, g], am_s.at[3, g], am_r.at[3, g])

    outs = []
    for p in range(NR):
        for g in range(GROUPS):
            dst = hg_ref.at[pl.ds((p // NX) * PROWS + g * 16, 16), pl.ds((p % NX) * CHIP, CHIP)]
            outs.append(pltpu.make_async_copy(og.at[p, g], dst, out_sem.at[p * GROUPS + g + NR + 1]))
            outs[-1].start()
    w_out.wait()
    for o in outs:
        o.wait()

    for rc in sent:
        rc.wait_send()
    for k in range(1, NR):
        g = (j + k) % NR

        @pl.when(g < GROUPS)
        def _():
            copy(fb.at[g], r2.at[j], f_s.at[k], f_r.at[k], second(g)).wait_send()

        @pl.when(j < GROUPS)
        def _():
            copy(og.at[i, j], og.at[i, j], g_s.at[k], g_r.at[j], second(g)).wait_send()


def body(hidden, out_weight, targets, token_weight):
    dma = pltpu.SemaphoreType.DMA
    vm = pltpu.VMEM
    loss, hg, wg = pl.pallas_call(
        kernel,
        name="fused_xent",
        out_shape=(
            jax.ShapeDtypeStruct((1, TOK), F32),
            jax.ShapeDtypeStruct((TOK, NX * CHIP), BF16),
            jax.ShapeDtypeStruct((WROWS, COLS), BF16),
        ),
        in_specs=[
            pl.BlockSpec(memory_space=pl.ANY),
            pl.BlockSpec(memory_space=pl.ANY),
            pl.BlockSpec(memory_space=vm),
            pl.BlockSpec(memory_space=vm),
        ],
        out_specs=(
            pl.BlockSpec(memory_space=vm),
            pl.BlockSpec(memory_space=pl.ANY),
            pl.BlockSpec(memory_space=pl.ANY),
        ),
        scratch_shapes=[
            vm((TOKP, NX * CHIP), BF16),
            vm((NX, CHIP, TOKP), BF16),
            vm((NX, CHIP, COLS), BF16),
            vm((TOK, COLS), F32),
            vm((TOK, COLS), F32),
            vm((TOK, COLS), F32),
            vm((8, TOKP), F32),
            vm((TOKP, 128), jnp.int32),
            vm((TOKP, 128), F32),
            vm((TOKP, 128), F32),
            vm((TOKP, 128), F32),
            vm((NR, 2, TOKP), F32),
            vm((NR, 2, TOKP), F32),
            vm((TOKP, COLS), BF16),
            vm((4, SUBS, PROWS, COLS), BF16),
            vm((4, SUBS, PROWS, COLS), BF16),
            vm((4, SUBS, PROWS, COLS), BF16),
            vm((4, SUBS, PROWS, COLS), BF16),
            vm((GROUPS, 16, CHIP), BF16),
            vm((NR, 16, CHIP), BF16),
            vm((NR, GROUPS, 16, CHIP), BF16),
            vm((NX, 2, WHALF, COLS), BF16),
            vm((NX, 2, WHALF, COLS), BF16),
            vm((6, WHALF, COLS), BF16),
            vm((6, WHALF, COLS), BF16),
            vm((WROWS, COLS), BF16),
            dma((2,)), dma((NR + 1 + NR * GROUPS,)),
            dma((13,)), dma((13,)),
            dma((2 * NR,)), dma((2 * NR,)),
            dma((4, SUBS)), dma((4, SUBS)),
            dma((4, SUBS)), dma((4, SUBS)),
            dma((NR,)), dma((NR,)),
            dma((NR,)), dma((GROUPS,)),
            dma((4, GROUPS)), dma((4, GROUPS)),
            dma((4, GROUPS)), dma((4, GROUPS)),
            dma((NX, 2)), dma((NX, 2)),
            dma((6,)), dma((6,)),
        ],
        compiler_params=pltpu.CompilerParams(
            collective_id=0, has_side_effects=True, vmem_limit_bytes=60 * 1024 * 1024
        ),
    )(hidden, out_weight, targets.reshape(1, TOK), token_weight.reshape(1, TOK))
    return loss.reshape(TOK), hg, wg


def solution(mesh):
    torus = Mesh(mesh.devices.reshape(NX, 2, NR, NR), ("x", "c", "y", "z"))
    dp, vocab = ("x", "c"), ("y", "z")
    in_specs = (P(dp, None), P(dp, vocab), P(dp), P(dp))
    out_specs = (P(dp), P(dp, None), P(dp, vocab))
    return jax.shard_map(body, mesh=torus, in_specs=in_specs, out_specs=out_specs, check_vma=False)
```

```python
import jax
import jax.numpy as jnp
from jax import lax
from jax.experimental import pallas as pl
from jax.experimental.pallas import tpu as pltpu
from jax.sharding import Mesh
from jax.sharding import PartitionSpec as P

MESH = pl.DeviceIdType.MESH
F32 = jnp.float32
BF16 = jnp.bfloat16

softcap = 30.0

NX = 4
NR = 8
TOK = 224
TOKP = 256
WROWS = 576
CHIP = 2 * WROWS
COLS = 384
WHALF = WROWS // 2
PROWS = TOK // 2
SUBS = CHIP // COLS
GROUPS = PROWS // 16
NT = (((1,), (1,)), ((), ()))
FAR_FIRST = (4, 3, 5, 2, 6, 1, 7, 0)
NEAR_FIRST = (0, 1, 7, 2, 6, 3, 5, 4)
UP4 = (4, 5, 6, 7)


def kernel(
    h_ref, w_ref, t_ref, tw_ref,
    loss_ref, og, wout,
    hv, ht, wf, acc, a1, a2, ab, pu, tin, win, rows, tcol, wcol, s128, t128, st1, st2, gk,
    sp, rp, sm, rm, fb, r2, ds_, dr, xs, xr,
    in_sem, w_s, w_r, st_s, st_r, p_s, p_r, m_s, m_r, f_s, f_r, g_s, g_r,
    ap_s, ap_r, am_s, am_r, d_s, d_r, x_s, x_r,
):
    x, c = lax.axis_index("x"), lax.axis_index("c")
    y, z = lax.axis_index("y"), lax.axis_index("z")
    xl, xr_, x2 = (x + NX - 1) % NX, (x + 1) % NX, (x + 2) % NX
    oc = 1 - c
    i = y * oc + z * c
    j = z * oc + y * c

    def first(n):
        return (x, c, n * oc + y * c, z * oc + n * c)

    def second(n):
        return (x, c, y * oc + n * c, n * oc + z * c)

    right, left, partner = (xr_, c, y, z), (xl, c, y, z), (x, oc, y, z)
    up, down = first((i + 1) % NR), first((i + NR - 1) % NR)

    def copy(src, dst, s, r, dev):
        return pltpu.make_async_remote_copy(
            src_ref=src, dst_ref=dst, send_sem=s, recv_sem=r, device_id=dev, device_id_type=MESH
        )

    def send(src, dst, s, r, dev):
        copy(src, dst, s, r, dev).start()

    def arrived(dst, s, r):
        copy(dst, dst, s, r, partner).wait_recv()

    def all_sent(refs, s, r):
        copy(refs, refs, s, r, partner).wait_send()

    own_rows = pl.ds(pl.multiple_of(c * WROWS, 32), WROWS)
    other_rows = pl.ds(pl.multiple_of(oc * WROWS, 32), WROWS)
    w_in = pltpu.make_async_copy(w_ref, wf.at[x, own_rows], in_sem.at[0])
    w_in.start()
    h_in = pltpu.make_async_copy(h_ref, hv.at[pl.ds(0, TOK)], in_sem.at[1])
    h_in.start()
    t_in = pltpu.make_async_copy(t_ref, tin, in_sem.at[2])
    t_in.start()
    tw_in = pltpu.make_async_copy(tw_ref, win, in_sem.at[3])
    tw_in.start()

    barrier = pltpu.get_barrier_semaphore()
    peers = [right, left, partner]
    for k in range(1, NR):
        peers.append(first((i + k) % NR))
        peers.append(second((j + k) % NR))
    for peer in peers:
        pl.semaphore_signal(barrier, inc=1, device_id=peer, device_id_type=MESH)
    pl.semaphore_wait(barrier, len(peers))

    def wpart(xx, cc, h):
        return wf.at[xx, pl.ds(pl.multiple_of(cc * WROWS + h * WHALF, 32), WHALF)]

    def wsend(xx, h, n, dev):
        send(wpart(xx, c, h), wpart(xx, c, h), w_s.at[0], w_r.at[n], dev)

    def wgot(xx, cc, h, n):
        arrived(wpart(xx, cc, h), w_s.at[0], w_r.at[n])

    w_in.wait()
    wsend(x, 0, 0, right)
    wsend(x, 1, 3, left)
    wsend(x, 1, 1, right)
    wsend(x, 0, 4, left)
    send(wf.at[x, own_rows], wf.at[x, own_rows], w_s.at[0], w_r.at[6], partner)

    t_in.wait()
    tw_in.wait()
    rows[...] = jnp.zeros_like(rows)
    rows[0:1, 0:TOK] = tin[...].astype(F32)
    rows[1:2, 0:TOK] = win[...]
    tcol[...] = jnp.broadcast_to(rows[0:1, :], (128, TOKP)).T.astype(jnp.int32)
    wcol[...] = jnp.broadcast_to(rows[1:2, :], (128, TOKP)).T
    pad = pl.ds(TOK, TOKP - TOK)
    s128[pad] = jnp.zeros((TOKP - TOK, 128), F32)
    t128[pad] = jnp.zeros((TOKP - TOK, 128), F32)
    gk[pad] = jnp.zeros((TOKP - TOK, COLS), BF16)
    hv[pad] = jnp.zeros((TOKP - TOK, NX * CHIP), BF16)
    h_in.wait()

    def part_logits(xx):
        at = pl.ds(pl.multiple_of(xx * CHIP, 128), CHIP)
        return jnp.dot(hv[pl.ds(0, TOK), at], wf[xx], preferred_element_type=F32)

    arrived(wf.at[x, other_rows], w_s.at[0], w_r.at[6])
    acc[...] = part_logits(x)

    @pl.loop(0, NX)
    def _(n):
        @pl.loop(0, CHIP // 128)
        def _(b):
            at = pl.ds(pl.multiple_of(n * CHIP + b * 128, 128), 128)
            ht[n, pl.ds(pl.multiple_of(b * 128, 128), 128), :] = hv[:, at].T

    wgot(xl, c, 0, 0)
    wsend(xl, 0, 2, right)
    wsend(xl, 0, 7, partner)
    wgot(xr_, c, 1, 3)
    wsend(xr_, 1, 5, left)
    wsend(xr_, 1, 8, partner)
    wgot(xl, c, 1, 1)
    wsend(xl, 1, 9, partner)
    wgot(xr_, c, 0, 4)
    wsend(xr_, 0, 10, partner)
    wgot(xl, oc, 0, 7)
    wgot(xl, oc, 1, 9)
    acc[...] += part_logits(xl)
    wgot(xr_, oc, 1, 8)
    wgot(xr_, oc, 0, 10)
    acc[...] += part_logits(xr_)
    wgot(x2, c, 0, 2)
    wsend(x2, 0, 11, partner)
    wgot(x2, c, 1, 5)
    wsend(x2, 1, 12, partner)
    wgot(x2, oc, 0, 11)
    wgot(x2, oc, 1, 12)
    acc[...] += part_logits(x2)

    first_col = (y * NR + z) * COLS
    used = COLS * NR * NR - COLS // 2

    @pl.loop(0, TOK // 16)
    def _(r):
        at = pl.ds(pl.multiple_of(r * 16, 16), 16)
        at2 = pl.ds(pl.multiple_of(TOK + r * 16, 16), 16)
        tgt, wgt = tcol[at], wcol[at]
        total, hits = jnp.zeros((16, 128), F32), jnp.zeros((16, 128), F32)
        for n in range(COLS // 128):
            lanes = pl.ds(n * 128, 128)
            ids = first_col + n * 128 + lax.broadcasted_iota(jnp.int32, (16, 128), 1)
            squash = jnp.tanh(acc[at, lanes] / softcap)
            capped = softcap * squash
            exps = jnp.where(ids < used, jnp.exp(capped), 0.0)
            hit = ids == tgt
            slope = wgt * (1.0 - squash * squash)
            grown, single = slope * exps, jnp.where(hit, slope, 0.0)
            a1[at, lanes] = grown
            a2[at, lanes] = single
            ab[at, lanes] = grown.astype(BF16)
            ab[at2, lanes] = single.astype(BF16)
            total += exps
            hits += jnp.where(hit, capped, 0.0)
        s128[at] = total
        t128[at] = hits

    st1[i, 0:1, :] = jnp.sum(s128[...].T, axis=0, keepdims=True)
    st1[i, 1:2, :] = jnp.sum(t128[...].T, axis=0, keepdims=True)

    def share(st, mine, dev, n):
        for k in FAR_FIRST[:-1]:
            send(st.at[mine], st.at[mine], st_s.at[n], st_r.at[n, k], dev((mine + k) % NR))

    def shared(st, mine, n):
        for k in NEAR_FIRST[1:]:
            arrived(st.at[(mine + NR - k) % NR], st_s.at[n], st_r.at[n, k])
        total = st[0]
        for k in range(1, NR):
            total += st[k]
        return total

    def products(lo):
        @pl.loop(0, 2 * SUBS)
        def _(n):
            b, at = lo + n // SUBS, pl.ds(pl.multiple_of((n % SUBS) * COLS, 128), COLS)
            pu[b, :, at] = lax.dot_general(ab[...], wf[b, at, :], NT, preferred_element_type=F32)

    share(st1, i, first, 0)
    products(0)
    st2[j] = shared(st1, i, 0)
    share(st2, j, second, 1)
    products(2)
    stats = shared(st2, j, 1)
    sums = stats[0:1, :]
    loss_ref[...] = jnp.log(sums[:, 0:TOK]) - stats[1:2, 0:TOK]
    s128[...] = jnp.broadcast_to(1.0 / sums, (128, TOKP)).T

    def chunk(p, g):
        row = (p // NX) * PROWS + g * 16
        at, at2 = pl.ds(pl.multiple_of(row, 16), 16), pl.ds(pl.multiple_of(TOK + row, 16), 16)
        inv = jnp.concatenate([s128[at]] * (CHIP // 128), axis=1)
        return pu[p % NX, at, :] * inv - pu[p % NX, at2, :]

    def hop(s, o, p, out, into, s_sem, r_sem, dev, adds):
        g = (j + o) % NR

        @pl.when(g < GROUPS)
        def _():
            val = chunk(p, g)
            if adds:
                arrived(into.at[s - 1, o], s_sem.at[0], r_sem.at[s - 1, o])
                val += into[s - 1, o].astype(F32)
            out[s, o] = val.astype(BF16)
            send(out.at[s, o], into.at[s, o], s_sem.at[min(s, 1)], r_sem.at[s, o], dev)

    def hop_up(s, o):
        hop(s, o, (i + 4 - s) % NR, sp, rp, p_s, p_r, up, s > 1 or (s == 1 and o in UP4))

    def hop_down(s, o):
        hop(s, o, (i + 4 + s) % NR, sm, rm, m_s, m_r, down, s > 1 or (s == 1 and o not in UP4))

    for o in FAR_FIRST:
        (hop_up if o in UP4 else hop_down)(0, o)
    for o in FAR_FIRST:
        (hop_down if o in UP4 else hop_up)(1, o)

    @pl.loop(0, TOK // 16)
    def _(r):
        at = pl.ds(pl.multiple_of(r * 16, 16), 16)
        inv = s128[at]
        for n in range(COLS // 128):
            lanes = pl.ds(n * 128, 128)
            gk[at, lanes] = (a1[at, lanes] * inv - a2[at, lanes]).astype(BF16)

    def term(xx, cc, h):
        a = ht[xx, pl.ds(pl.multiple_of(cc * WROWS + h * WHALF, 32), WHALF), :]
        return jnp.dot(a, gk[...], preferred_element_type=F32)

    def give(xx, h):
        ds_[xx, h] = term(xx, oc, h).astype(BF16)
        send(ds_.at[xx, h], dr.at[xx, h], d_s.at[0], d_r.at[xx, h], partner)

    def chip_term(xx, h):
        val = term(xx, c, h)
        arrived(dr.at[xx, h], d_s.at[0], d_r.at[xx, h])
        return val + dr[xx, h].astype(F32)

    def pass_on(n, val, dev):
        xs[n] = val.astype(BF16)
        send(xs.at[n], xr.at[n], x_s.at[0], x_r.at[n], dev)

    def got(n):
        arrived(xr.at[n], x_s.at[0], x_r.at[n])
        return xr[n].astype(F32)

    give(x2, 0)
    give(x2, 1)
    for o in FAR_FIRST:
        (hop_up if o in UP4 else hop_down)(1, o)
    give(xr_, 1)
    give(xl, 0)
    for o in FAR_FIRST:
        hop_up(2, o)
        hop_down(2, o)
    pass_on(0, chip_term(x2, 0), right)
    pass_on(3, chip_term(x2, 1), left)
    for o in FAR_FIRST:
        hop_up(3, o)
        hop_down(3, o)
    pass_on(1, chip_term(xr_, 1), right)
    pass_on(4, chip_term(xl, 0), left)

    for o in FAR_FIRST:
        g = (j + o) % NR

        @pl.when(g < GROUPS)
        def _():
            val = chunk(i, g)
            arrived(rp.at[3, o], p_s.at[0], p_r.at[3, o])
            arrived(rm.at[3, o], m_s.at[0], m_r.at[3, o])
            val += rp[3, o].astype(F32) + rm[3, o].astype(F32)
            fb[o] = val.astype(BF16)
            if o:
                send(fb.at[o], r2.at[o], f_s.at[0], f_r.at[o], second(g))

    give(xr_, 0)
    give(xl, 1)
    give(x, 0)
    give(x, 1)

    def og_at(p, g):
        return og.at[p, pl.ds(pl.multiple_of(g * 16, 16), 16)]

    @pl.when(j < GROUPS)
    def _():
        total = fb[0].astype(F32)
        for o in NEAR_FIRST[1:]:
            arrived(r2.at[o], f_s.at[0], f_r.at[o])
            total += r2[o].astype(F32)
        og[i, pl.ds(pl.multiple_of(j * 16, 16), 16)] = total.astype(BF16)
        for k in FAR_FIRST[:-1]:
            send(og_at(i, j), og_at(i, j), g_s.at[0], g_r.at[NR - k], second((j + k) % NR))

    def ring(s, o, g, p_up, p_down):
        if s < 3 or o in UP4:
            send(og_at(p_up, g), og_at(p_up, g), ap_s.at[s // 3], ap_r.at[s, o], up)
        if s < 3 or o not in UP4:
            send(og_at(p_down, g), og_at(p_down, g), am_s.at[s // 3], am_r.at[s, o], down)

    for o in NEAR_FIRST:
        g = (j + o) % NR

        @pl.when(g < GROUPS)
        def _():
            if o:
                arrived(og_at(i, g), g_s.at[0], g_r.at[o])
            ring(0, o, g, i, i)

    pass_on(2, chip_term(xr_, 0) + got(0), right)
    pass_on(5, chip_term(xl, 1) + got(3), left)

    for s in range(1, 4):
        p_up, p_down = (i + NR - s) % NR, (i + s) % NR
        for o in NEAR_FIRST:
            g = (j + o) % NR

            @pl.when(g < GROUPS)
            def _():
                arrived(og_at(p_up, g), ap_s.at[0], ap_r.at[s - 1, o])
                arrived(og_at(p_down, g), am_s.at[0], am_r.at[s - 1, o])
                ring(s, o, g, p_up, p_down)

    wout[pl.ds(0, WHALF)] = (chip_term(x, 0) + got(2) + got(4)).astype(BF16)
    wout[pl.ds(WHALF, WHALF)] = (chip_term(x, 1) + got(5) + got(1)).astype(BF16)

    far = (i + 4) % NR
    for o in NEAR_FIRST:
        g = (j + o) % NR

        @pl.when(g < GROUPS)
        def _():
            if o in UP4:
                arrived(og_at(far, g), ap_s.at[0], ap_r.at[3, o])
            else:
                arrived(og_at(far, g), am_s.at[0], am_r.at[3, o])

    all_sent(wf.at[:, pl.ds(0, 14 * WHALF // NX)], w_s.at[0], w_r.at[0])
    all_sent(st1.at[pl.ds(0, NR - 1)], st_s.at[0], st_r.at[0, 0])
    all_sent(st2.at[pl.ds(0, NR - 1)], st_s.at[1], st_r.at[1, 0])
    all_sent(ds_, d_s.at[0], d_r.at[0, 0])
    all_sent(xs, x_s.at[0], x_r.at[0])
    for ring_s, ring_r in ((p_s, p_r), (m_s, m_r)):
        all_sent(sp.at[pl.ds(0, 3), pl.ds(0, GROUPS)], ring_s.at[1], ring_r.at[0, 0])
    for ring_s, ring_r in ((ap_s, ap_r), (am_s, am_r)):
        all_sent(sp.at[pl.ds(0, 3), pl.ds(0, GROUPS)], ring_s.at[0], ring_r.at[0, 0])

    def fourth(n_up, n_down):
        all_sent(sp.at[0, pl.ds(0, n_up)], p_s.at[0], p_r.at[0, 0])
        all_sent(sp.at[0, pl.ds(0, n_down)], m_s.at[0], m_r.at[0, 0])
        all_sent(sp.at[0, pl.ds(0, n_up)], ap_s.at[1], ap_r.at[0, 0])
        all_sent(sp.at[0, pl.ds(0, n_down)], am_s.at[1], am_r.at[0, 0])

    @pl.when(j < 4)
    def _():
        fourth(3, 4)

    @pl.when(j >= 4)
    def _():
        fourth(4, 3)

    @pl.when(j < GROUPS)
    def _():
        all_sent(fb.at[pl.ds(0, NR - 2)], f_s.at[0], f_r.at[0])
        all_sent(fb.at[pl.ds(0, NR - 1)], g_s.at[0], g_r.at[0])

    @pl.when(j >= GROUPS)
    def _():
        all_sent(fb.at[pl.ds(0, NR - 1)], f_s.at[0], f_r.at[0])


def finish(loss_in, og, w_in, loss_ref, hg_ref, wg_ref, sem):
    copies = [
        pltpu.make_async_copy(
            og.at[p], hg_ref.at[pl.ds((p // NX) * PROWS, PROWS), pl.ds((p % NX) * CHIP, CHIP)], sem.at[p]
        )
        for p in range(NR)
    ]
    copies.append(pltpu.make_async_copy(w_in, wg_ref, sem.at[NR]))
    copies.append(pltpu.make_async_copy(loss_in, loss_ref, sem.at[NR + 1]))
    for one in copies:
        one.start()
    for one in copies:
        one.wait()


def body(hidden, out_weight, targets, token_weight):
    dma = pltpu.SemaphoreType.DMA
    vm = pltpu.VMEM
    anywhere, inside = pl.BlockSpec(memory_space=pl.ANY), pl.BlockSpec(memory_space=vm)
    chunks = vm((4, NR, 16, CHIP), BF16)
    loss, og, wout = pl.pallas_call(
        kernel,
        name="fused_xent",
        out_shape=(
            vm((1, TOK), F32),
            vm((NR, PROWS, CHIP), BF16),
            vm((WROWS, COLS), BF16),
        ),
        in_specs=[anywhere] * 4,
        out_specs=(inside,) * 3,
        scratch_shapes=[
            vm((TOKP, NX * CHIP), BF16),
            vm((NX, CHIP, TOKP), BF16),
            vm((NX, CHIP, COLS), BF16),
            vm((TOK, COLS), F32),
            vm((TOK, COLS), F32),
            vm((TOK, COLS), F32),
            vm((2 * TOK, COLS), BF16),
            vm((NX, 2 * TOK, CHIP), F32),
            vm((1, TOK), jnp.int32),
            vm((1, TOK), F32),
            vm((8, TOKP), F32),
            vm((TOKP, 128), jnp.int32),
            vm((TOKP, 128), F32),
            vm((TOKP, 128), F32),
            vm((TOKP, 128), F32),
            vm((NR, 2, TOKP), F32),
            vm((NR, 2, TOKP), F32),
            vm((TOKP, COLS), BF16),
            chunks, chunks, chunks, chunks,
            vm((NR, 16, CHIP), BF16),
            vm((NR, 16, CHIP), BF16),
            vm((NX, 2, WHALF, COLS), BF16),
            vm((NX, 2, WHALF, COLS), BF16),
            vm((6, WHALF, COLS), BF16),
            vm((6, WHALF, COLS), BF16),
            dma((4,)),
            dma((1,)), dma((13,)),
            dma((2,)), dma((2, NR)),
            dma((2,)), dma((4, NR)),
            dma((2,)), dma((4, NR)),
            dma((1,)), dma((NR,)),
            dma((1,)), dma((NR,)),
            dma((2,)), dma((4, NR)),
            dma((2,)), dma((4, NR)),
            dma((1,)), dma((NX, 2)),
            dma((1,)), dma((6,)),
        ],
        compiler_params=pltpu.CompilerParams(
            collective_id=0, has_side_effects=True, vmem_limit_bytes=48 * 1024 * 1024
        ),
    )(*[
        pltpu.with_memory_space_constraint(one, pltpu.HBM)
        for one in (hidden, out_weight, targets.reshape(1, TOK), token_weight.reshape(1, TOK))
    ])
    loss, hg, wg = pl.pallas_call(
        finish,
        name="to_hbm",
        out_shape=(
            jax.ShapeDtypeStruct((1, TOK), F32),
            jax.ShapeDtypeStruct((TOK, NX * CHIP), BF16),
            jax.ShapeDtypeStruct((WROWS, COLS), BF16),
        ),
        in_specs=[inside] * 3,
        out_specs=(anywhere,) * 3,
        scratch_shapes=[dma((NR + 2,))],
    )(*[pltpu.with_memory_space_constraint(one, pltpu.VMEM) for one in (loss, og, wout)])
    return loss.reshape(TOK), hg, wg


def solution(mesh):
    torus = Mesh(mesh.devices.reshape(NX, 2, NR, NR), ("x", "c", "y", "z"))
    dp, vocab = ("x", "c"), ("y", "z")
    in_specs = (P(dp, None), P(dp, vocab), P(dp), P(dp))
    out_specs = (P(dp), P(dp, None), P(dp, vocab))
    return jax.shard_map(body, mesh=torus, in_specs=in_specs, out_specs=out_specs, check_vma=False)
```
